8 devices in a mesh: dp: 1 (over z), tp: 2 (over y), ep: 4 (over x, core).
Axes of the slice: x: 2, y: 2, z: 1, core: 2. Of those that a mesh axis runs over, the one named last changes fastest.
Arguments:
- tokens: bfloat16 [2048, 2048], P(('dp', 'ep', 'tp'))
- expert_ids: int32 [2048, 6], P(('dp', 'ep', 'tp'))
- gates: float32 [2048, 6], P(('dp', 'ep', 'tp'))
- w_gate: bfloat16 [64, 2048, 1408], P('ep', None, 'tp')
- w_up: bfloat16 [64, 2048, 1408], P('ep', None, 'tp')
- w_down: bfloat16 [64, 1408, 2048], P('ep', 'tp')
Outputs:
- output: bfloat16 [2048, 2048], P(('dp', 'ep', 'tp'))
All inputs are finite; a program needn't handle non-finite values.
Results may differ from the reference program's by a relative error of at most 0.00123.
Values are sent between devices in bfloat16 or wider.
A program may use at most 1 GiB of HBM per device.

```python
import jax
import jax.numpy as jnp
from jax import lax

TOKENS_DEV = 256
HIDDEN = 2048
EXPERT_FF = 1408
EXPERTS = 64
TOP_K = 6
EP_SIZE = 4
TP_SIZE = 2

TOKENS = TOKENS_DEV * EP_SIZE * TP_SIZE
SPREAD = min(TOP_K, EP_SIZE)


def routing_ids(base_key):
    group_devices = EP_SIZE * TP_SIZE
    class_rows = TOKENS_DEV // EP_SIZE
    local_count = EXPERTS // EP_SIZE
    key_rows, key_target, key_rot = jax.random.split(base_key, 3)
    row_order = jax.vmap(lambda sub_key: jax.random.permutation(sub_key, TOKENS_DEV))(jax.random.split(key_rows, group_devices))
    ep_order = jax.vmap(lambda sub_key: jax.random.permutation(sub_key, EP_SIZE))(jax.random.split(key_target, group_devices))
    rotation = jax.random.randint(key_rot, (), 0, local_count)
    slots = jnp.arange(TOP_K)
    ep_class = row_order % EP_SIZE
    within = row_order // EP_SIZE + jnp.arange(group_devices)[:, None] * class_rows
    place = (ep_class[:, :, None] + slots % SPREAD) % EP_SIZE
    target_ep = jax.vmap(lambda order_row, place_rows: order_row[place_rows])(ep_order, place)
    local_slot = (within[:, :, None] + slots // SPREAD + rotation) % local_count
    return (target_ep * local_count + local_slot).astype(jnp.int32).reshape(TOKENS, TOP_K)


def setup_inputs(seed: int = 0, part: int = 0) -> dict:
    base_key = jax.random.key(seed)
    key_gate_w, key_up_w, key_down_w, key_part = jax.random.split(base_key, 4)
    key_tokens, key_ids, key_gates = jax.random.split(jax.random.fold_in(key_part, part), 3)
    tokens = jax.random.normal(key_tokens, (TOKENS, HIDDEN), jnp.float32).astype(jnp.bfloat16)
    expert_ids = routing_ids(key_ids)
    gates = jax.random.uniform(key_gates, (TOKENS, TOP_K), jnp.float32, 0.5, 1.5)
    w_gate = (jax.random.normal(key_gate_w, (EXPERTS, HIDDEN, EXPERT_FF), jnp.float32) * HIDDEN ** -0.5).astype(jnp.bfloat16)
    w_up = (jax.random.normal(key_up_w, (EXPERTS, HIDDEN, EXPERT_FF), jnp.float32) * HIDDEN ** -0.5).astype(jnp.bfloat16)
    w_down = (jax.random.normal(key_down_w, (EXPERTS, EXPERT_FF, HIDDEN), jnp.float32) * EXPERT_FF ** -0.5).astype(jnp.bfloat16)
    return {"tokens": tokens, "expert_ids": expert_ids, "gates": gates, "w_gate": w_gate, "w_up": w_up, "w_down": w_down}


def reference(tokens, expert_ids, gates, w_gate, w_up, w_down):
    load = TOKENS * TOP_K // EXPERTS
    order = jnp.argsort(expert_ids.reshape(-1), stable=True).reshape(EXPERTS, load)
    row_index = order // TOP_K
    gate_sorted = gates.reshape(-1)[order]

    def expert_out(operands):
        rows_in, gate_in, gate_mat, up_mat, down_mat = operands
        x_rows = tokens[rows_in]
        hidden_gate = jnp.dot(x_rows, gate_mat, preferred_element_type=jnp.float32)
        hidden_up = jnp.dot(x_rows, up_mat, preferred_element_type=jnp.float32)
        act_rows = (jax.nn.silu(hidden_gate) * hidden_up).astype(jnp.bfloat16)
        out_rows = jnp.dot(act_rows, down_mat, preferred_element_type=jnp.float32)
        return out_rows * gate_in[:, None]

    weighted = lax.map(expert_out, (row_index, gate_sorted, w_gate, w_up, w_down))
    summed = jax.ops.segment_sum(weighted.reshape(-1, HIDDEN), row_index.reshape(-1), num_segments=TOKENS)
    return summed.astype(jnp.bfloat16)
```

```python
import functools

import jax
import jax.numpy as jnp
from jax import lax
from jax.experimental import pallas as pl
from jax.experimental.pallas import tpu as pltpu
from jax.sharding import PartitionSpec as P

MESH = pl.DeviceIdType.MESH
F32 = jnp.float32
BF16 = jnp.bfloat16

ROWS = 256
HALF = ROWS // 2
NDEV = 8
TOPC = 3
COLS = 1024


def _dot(a, b):
    return jnp.dot(a, b, preferred_element_type=F32)


def _dot_t(a, b):
    return lax.dot_general(a, b, (((1,), (1,)), ((), ())), preferred_element_type=F32)


def _coords():
    ep = lax.axis_index("ep")
    tp = lax.axis_index("tp")
    x = ep // 2
    k = ep - 2 * x
    return ep, tp, x, k


def _remote(src, dst, ssem, rsem, ep, tp):
    return pltpu.make_async_remote_copy(
        src_ref=src, dst_ref=dst, send_sem=ssem, recv_sem=rsem,
        device_id={"ep": ep, "tp": tp}, device_id_type=MESH)


def dispatch_kernel(nbuf, tok_ref, meta_ref, wg_hbm, wu_hbm, h_hbm, cidx_ref, gk_ref,
                    rb, meta_all, x_ref, wg_buf, wu_buf, h_buf, rank_ref, rankg_ref,
                    wsem, hsem, tsend, trecv, msend, mrecv):
    experts, load = x_ref.shape[0], x_ref.shape[1]
    hidden = x_ref.shape[2]
    ff = wg_buf.shape[1]
    ep, tp, x, k = _coords()
    me = ep * 2 + tp
    sib = 2 * x + (1 - k)
    xn = 2 * (1 - x) + k
    yt = 1 - tp

    def weights(e, slot):
        return (pltpu.make_async_copy(wg_hbm.at[e], wg_buf.at[slot], wsem.at[0, slot]),
                pltpu.make_async_copy(wu_hbm.at[e], wu_buf.at[slot], wsem.at[1, slot]))

    for e in range(nbuf):
        for cp in weights(e, e):
            cp.start()

    others = []
    for step in range(1, NDEV):
        d = lax.rem(me + step, NDEV)
        others.append((d // 2, d % 2, step))
    barrier = pltpu.get_barrier_semaphore()
    for oe, ot, _ in others:
        pl.semaphore_signal(barrier, inc=1, device_id={"ep": oe, "tp": ot}, device_id_type=MESH)
    pl.semaphore_wait(barrier, NDEV - 1)

    metas = []
    for oe, ot, step in others:
        cp = _remote(meta_ref, meta_all.at[me], msend.at[step - 1], mrecv.at[step - 1], oe, ot)
        cp.start()
        metas.append(cp)

    top, bot = pl.ds(0, HALF), pl.ds(HALF, HALF)
    own = (tok_ref.at[top], tok_ref.at[bot])
    x0 = _remote(own[0], rb.at[1, top], tsend.at[0], trecv.at[1, 0], xn, tp)
    y1 = _remote(own[1], rb.at[1, bot], tsend.at[1], trecv.at[1, 1], ep, yt)
    x1 = _remote(own[1], rb.at[2, top], tsend.at[2], trecv.at[2, 0], xn, tp)
    y0 = _remote(own[0], rb.at[2, bot], tsend.at[3], trecv.at[2, 1], ep, yt)
    fy = _remote(rb.at[1, top], rb.at[3, top], tsend.at[4], trecv.at[3, 0], ep, yt)
    fx = _remote(rb.at[1, bot], rb.at[3, bot], tsend.at[5], trecv.at[3, 1], xn, tp)
    sibs = [_remote(tok_ref if g == 0 else rb.at[g], rb.at[4 + g], tsend.at[6 + g],
                    trecv.at[4 + g, 0], sib, tp) for g in range(4)]
    for cp in (x0, y1, x1, y0, sibs[0]):
        cp.start()

    meta_all[me] = meta_ref[...]
    for cp in metas:
        cp.wait_recv()
    row_i = lax.broadcasted_iota(jnp.int32, (ROWS, ROWS), 0)
    col_i = lax.broadcasted_iota(jnp.int32, (ROWS, ROWS), 1)
    before = jnp.where(row_i < col_i, 1.0, 0.0).astype(BF16)
    e_row = lax.broadcasted_iota(jnp.int32, (experts, ROWS), 0)
    lower = jnp.where(lax.broadcasted_iota(jnp.int32, (experts, experts), 1)
                      < lax.broadcasted_iota(jnp.int32, (experts, experts), 0), 1.0, 0.0).astype(BF16)
    e_global = (e_row + ep * experts).astype(F32)
    e_base = e_row.astype(F32) * float(load)
    base = jnp.zeros((experts, 1), F32)
    for b in range(NDEV):
        ind = jnp.zeros((experts, ROWS), F32)
        gate = jnp.zeros((experts, ROWS), F32)
        for j in range(6):
            hit = meta_all[b, j:j + 1, :] == e_global
            ind = jnp.where(hit, 1.0, ind)
            gate = jnp.where(hit, meta_all[b, 8 + j:9 + j, :], gate)
        ind16 = ind.astype(BF16)
        rank = _dot(ind16, before) + base
        base = base + jnp.sum(ind, axis=1, keepdims=True)
        pos = _dot(lower, ind16)
        rank_ref[b] = jnp.where(ind > 0.5, rank, -1.0)
        slot = e_base + rank
        for c in range(TOPC):
            sel = (ind > 0.5) & (pos == float(c))
            idx = jnp.sum(jnp.where(sel, slot, 0.0), axis=0, keepdims=True)
            cidx_ref[c:c + 1, b * ROWS:(b + 1) * ROWS] = idx.astype(jnp.int32)
            gk_ref[c:c + 1, b * ROWS:(b + 1) * ROWS] = jnp.sum(jnp.where(sel, gate, 0.0), axis=0, keepdims=True)
    for s in range(2):
        kk = k if s == 0 else 1 - k
        b_own = (2 * x + kk) * 2 + tp
        b_x = (2 * (1 - x) + kk) * 2 + tp
        b_y = (2 * x + kk) * 2 + yt
        b_d = (2 * (1 - x) + kk) * 2 + yt
        rankg_ref[4 * s] = rank_ref[b_own]
        rankg_ref[4 * s + 1, :, 0:HALF] = rank_ref[b_x, :, 0:HALF]
        rankg_ref[4 * s + 1, :, HALF:ROWS] = rank_ref[b_y, :, HALF:ROWS]
        rankg_ref[4 * s + 2, :, 0:HALF] = rank_ref[b_x, :, HALF:ROWS]
        rankg_ref[4 * s + 2, :, HALF:ROWS] = rank_ref[b_y, :, 0:HALF]
        rankg_ref[4 * s + 3] = rank_ref[b_d]

    def one_hot(q, e):
        want = lax.broadcasted_iota(jnp.int32, (load, ROWS), 0).astype(F32)
        return jnp.where(want == rankg_ref[q, pl.ds(e, 1), :], 1.0, 0.0).astype(BF16)

    def gather(e, g):
        oh0, oh1 = one_hot(g, e), one_hot(4 + g, e)
        for n in range(0, hidden, 512):
            cols = pl.ds(n, 512)
            left = tok_ref[:, cols] if g == 0 else rb[g, :, cols]
            got = (_dot(oh0, left) + _dot(oh1, rb[4 + g, :, cols])).astype(BF16)
            if g == 0:
                x_ref[e, :, cols] = got
            else:
                x_ref[e, :, cols] = x_ref[e, :, cols] + got

    def gather_all(g):
        def body(e, carry):
            gather(e, g)
            return carry
        lax.fori_loop(0, experts, body, 0)

    sibs[0].wait_recv()
    gather_all(0)
    x0.wait_recv()
    fy.start()
    y1.wait_recv()
    fx.start()
    sibs[1].start()
    sibs[1].wait_recv()
    gather_all(1)
    x1.wait_recv()
    y0.wait_recv()
    sibs[2].start()
    sibs[2].wait_recv()
    gather_all(2)
    fy.wait_recv()
    fx.wait_recv()
    sibs[3].start()
    sibs[3].wait_recv()

    def expert(e, carry):
        slot = lax.rem(e, nbuf)
        gather(e, 3)
        for cp in weights(e, slot):
            cp.wait()
        for n0, n1 in ((0, 256), (256, 512), (512, ff)):
            a = _dot_t(wg_buf[slot, n0:n1, :], x_ref[e])
            b = _dot_t(wu_buf[slot, n0:n1, :], x_ref[e])
            h_buf[e, :, n0:n1] = (a * jax.nn.sigmoid(a) * b).T.astype(BF16)
        pltpu.make_async_copy(h_buf.at[e], h_hbm.at[e], hsem.at[e]).start()

        @pl.when(e + nbuf < experts)
        def _():
            for cp in weights(e + nbuf, slot):
                cp.start()
        return carry

    lax.fori_loop(0, experts, expert, 0)
    for e in range(experts):
        pltpu.make_async_copy(h_buf.at[e], h_hbm.at[e], hsem.at[e]).wait()
    for cp in metas + [x0, y1, x1, y0, fy, fx] + sibs:
        cp.wait_send()


def return_kernel(nbuf, h_ref, wd_hbm, cidx_ref, gk_ref, out_ref,
                  wd_buf, o_ref, psib, pown, r0, r1, r2,
                  wsem, s0, v0, s1, v1, s2, v2):
    experts, load = h_ref.shape[0], h_ref.shape[1]
    ncol = wd_hbm.shape[2] // COLS
    ep, tp, x, k = _coords()
    sib = 2 * x + (1 - k)
    xn = 2 * (1 - x) + k
    yt = 1 - tp

    def weights(i, slot):
        c, e = i // experts, i % experts
        cols = pl.ds(pl.multiple_of(c * COLS, COLS), COLS)
        return pltpu.make_async_copy(wd_hbm.at[e, :, cols], wd_buf.at[slot], wsem.at[slot])

    for i in range(nbuf):
        weights(i, i).start()

    barrier = pltpu.get_barrier_semaphore()
    for oe, ot in ((sib, tp), (xn, tp), (ep, yt)):
        pl.semaphore_signal(barrier, inc=1, device_id={"ep": oe, "tp": ot}, device_id_type=MESH)
    pl.semaphore_wait(barrier, 3)

    def down(c):
        def body(e, carry):
            i = c * experts + e
            slot = lax.rem(i, nbuf)
            weights(i, slot).wait()
            for n in range(0, COLS, 256):
                o = _dot(h_ref[e], wd_buf[slot, :, n:n + 256])
                for j in range(2):
                    o_ref[pl.ds(e * load, load), n // 128 + j, :] = o[:, j * 128:(j + 1) * 128]

            @pl.when(i + nbuf < ncol * experts)
            def _():
                weights(i + nbuf, slot).start()
            return carry
        lax.fori_loop(0, experts, body, 0)

    unroll = 8

    def combine(dst, blk):
        def body(i, carry):
            for u in range(unroll):
                r = i * unroll + u
                t = blk * ROWS + r
                v = None
                for c in range(TOPC):
                    term = o_ref[cidx_ref[c, t]] * gk_ref[c, t]
                    v = term if v is None else v + term
                dst[pl.ds(pl.multiple_of(r * 8, 8), 8), :] = v
            return carry
        lax.fori_loop(0, ROWS // unroll, body, 0)

    tile = 256

    def add_into(dst, src, rows):
        def body(i, carry):
            at = pl.ds(pl.multiple_of(i * tile, tile), tile)
            dst[at, :] = dst[at, :] + src[at, :]
            return carry
        lax.fori_loop(0, rows // tile, body, 0)

    lo, hi = pl.ds(0, HALF * 8), pl.ds(HALF * 8, HALF * 8)

    def block(g, kk):
        xd = x if g < 2 else 1 - x
        yd = tp if g % 2 == 0 else 1 - tp
        return (2 * xd + kk) * 2 + yd

    stage0 = {(c, g): _remote(psib.at[c, g], r0.at[c, g], s0.at[c, g], v0.at[c, g], sib, tp)
              for c in range(ncol) for g in range(4)}
    stage1 = {}
    stage2 = {}
    for c in range(ncol):
        for d in range(2):
            stage1[c, 0, d] = _remote(pown.at[c, 2 + d, lo], r1.at[c, 0, d], s1.at[c, 0, d], v1.at[c, 0, d], xn, tp)
            stage1[c, 1, d] = _remote(pown.at[c, 1 + 2 * d, hi], r1.at[c, 1, d], s1.at[c, 1, d], v1.at[c, 1, d], ep, yt)
        stage2[c, 0] = _remote(pown.at[c, 1, lo], r2.at[c, 0], s2.at[c, 0], v2.at[c, 0], ep, yt)
        stage2[c, 1] = _remote(pown.at[c, 2, hi], r2.at[c, 1], s2.at[c, 1], v2.at[c, 1], xn, tp)

    def merge(c, g):
        combine(pown.at[c, g], block(g, k))
        stage0[c, g].wait_recv()
        add_into(pown.at[c, g], r0.at[c, g], ROWS * 8)

    for c in range(ncol):
        down(c)
        for g in (3, 2):
            combine(psib.at[c, g], block(g, 1 - k))
            stage0[c, g].start()
        merge(c, 3)
        stage1[c, 0, 1].start()
        stage1[c, 1, 1].start()
        combine(psib.at[c, 1], block(1, 1 - k))
        stage0[c, 1].start()
        merge(c, 2)
        stage1[c, 0, 0].start()
        combine(psib.at[c, 0], block(0, 1 - k))
        stage0[c, 0].start()
        merge(c, 1)
        stage1[c, 1, 0].start()
        merge(c, 0)
    for c in range(ncol):
        stage1[c, 0, 1].wait_recv()
        add_into(pown.at[c, 1, lo], r1.at[c, 0, 1], HALF * 8)
        stage2[c, 0].start()
        stage1[c, 1, 1].wait_recv()
        add_into(pown.at[c, 2, hi], r1.at[c, 1, 1], HALF * 8)
        stage2[c, 1].start()
    for c in range(ncol):
        for half in range(2):
            stage1[c, half, 0].wait_recv()
            add_into(pown.at[c, 0, lo if half == 0 else hi], r1.at[c, half, 0], HALF * 8)
    for c in range(ncol):
        for half in range(2):
            stage2[c, half].wait_recv()

            def body(i, carry, c=c, half=half):
                row = half * HALF + i * 16
                for j in range(8):
                    parts = []
                    for q in range(2):
                        at = (i * 16 + q * 8) * 8 + j
                        parts.append(pown[c, 0, pl.ds(half * HALF * 8 + at, 8, stride=8), :]
                                     + r2[c, half, pl.ds(at, 8, stride=8), :])
                    val = jnp.concatenate(parts, axis=0).astype(BF16)
                    out_ref[pl.ds(pl.multiple_of(row, 16), 16), c * COLS + j * 128:c * COLS + (j + 1) * 128] = val
                return carry
            lax.fori_loop(0, HALF // 16, body, 0)
    for cp in list(stage0.values()) + list(stage1.values()) + list(stage2.values()):
        cp.wait_send()


def solution(mesh):
    row_spec = P(("dp", "ep", "tp"), None)

    def local_layer(tokens, expert_ids, gates, w_gate, w_up, w_down):
        experts, hidden, ff = w_gate.shape
        load = ROWS * NDEV * expert_ids.shape[1] // (experts * 4)
        pad = ((0, 2), (0, 0))
        meta = jnp.concatenate([jnp.pad(expert_ids.astype(F32).T, pad), jnp.pad(gates.T, pad)], axis=0)
        nbuf = 4
        vm = pl.BlockSpec(memory_space=pltpu.VMEM)
        hbm = pl.BlockSpec(memory_space=pl.ANY)
        h, cidx, gk = pl.pallas_call(
            functools.partial(dispatch_kernel, nbuf),
            out_shape=(jax.ShapeDtypeStruct((experts, load, ff), BF16),
                       jax.ShapeDtypeStruct((TOPC, ROWS * NDEV), jnp.int32),
                       jax.ShapeDtypeStruct((TOPC, ROWS * NDEV), F32)),
            in_specs=[vm, vm, hbm, hbm],
            out_specs=(hbm, vm, vm),
            scratch_shapes=[
                pltpu.VMEM((8, ROWS, hidden), BF16),
                pltpu.VMEM((NDEV, 16, ROWS), F32),
                pltpu.VMEM((experts, load, hidden), BF16),
                pltpu.VMEM((nbuf, ff, hidden), BF16),
                pltpu.VMEM((nbuf, ff, hidden), BF16),
                pltpu.VMEM((experts, load, ff), BF16),
                pltpu.VMEM((NDEV, experts, ROWS), F32),
                pltpu.VMEM((8, experts, ROWS), F32),
                pltpu.SemaphoreType.DMA((2, nbuf)),
                pltpu.SemaphoreType.DMA((experts,)),
                pltpu.SemaphoreType.DMA((10,)),
                pltpu.SemaphoreType.DMA((8, 2)),
                pltpu.SemaphoreType.DMA((NDEV - 1,)),
                pltpu.SemaphoreType.DMA((NDEV - 1,)),
            ],
            compiler_params=pltpu.CompilerParams(collective_id=0, has_side_effects=True, vmem_limit_bytes=63 * 2**20),
            name="dispatch_up",
        )(tokens, meta, jnp.swapaxes(w_gate, 1, 2), jnp.swapaxes(w_up, 1, 2))

        nbuf2 = 6
        ncol = hidden // COLS
        sm = pl.BlockSpec(memory_space=pltpu.SMEM)
        return pl.pallas_call(
            functools.partial(return_kernel, nbuf2),
            out_shape=jax.ShapeDtypeStruct((ROWS, hidden), BF16),
            in_specs=[vm, hbm, sm, sm],
            out_specs=vm,
            scratch_shapes=[
                pltpu.VMEM((nbuf2, ff, COLS), BF16),
                pltpu.VMEM((experts * load, 8, 128), F32),
                pltpu.VMEM((ncol, 4, ROWS * 8, 128), F32),
                pltpu.VMEM((ncol, 4, ROWS * 8, 128), F32),
                pltpu.VMEM((ncol, 4, ROWS * 8, 128), F32),
                pltpu.VMEM((ncol, 2, 2, HALF * 8, 128), F32),
                pltpu.VMEM((ncol, 2, HALF * 8, 128), F32),
                pltpu.SemaphoreType.DMA((nbuf2,)),
                pltpu.SemaphoreType.DMA((ncol, 4)),
                pltpu.SemaphoreType.DMA((ncol, 4)),
                pltpu.SemaphoreType.DMA((ncol, 2, 2)),
                pltpu.SemaphoreType.DMA((ncol, 2, 2)),
                pltpu.SemaphoreType.DMA((ncol, 2)),
                pltpu.SemaphoreType.DMA((ncol, 2)),
            ],
            compiler_params=pltpu.CompilerParams(collective_id=1, has_side_effects=True, vmem_limit_bytes=63 * 2**20),
            name="down_return",
        )(h, w_down, cidx, gk)

    return jax.shard_map(local_layer, mesh=mesh, in_specs=(row_spec, row_spec, row_spec, P("ep", None, "tp"), P("ep", None, "tp"), P("ep", "tp", None)), out_specs=row_spec, check_vma=False)
```

```python
import functools

import jax
import jax.numpy as jnp
from jax import lax
from jax.experimental import pallas as pl
from jax.experimental.pallas import tpu as pltpu
from jax.sharding import PartitionSpec as P

MESH = pl.DeviceIdType.MESH
F32 = jnp.float32
BF16 = jnp.bfloat16

ROWS = 256
HALF = ROWS // 2
NDEV = 8
TOPC = 3
COLS = 1024


def _dot(a, b):
    return jnp.dot(a, b, preferred_element_type=F32)


def _dot_t(a, b):
    return lax.dot_general(a, b, (((1,), (1,)), ((), ())), preferred_element_type=F32)


def _coords():
    ep = lax.axis_index("ep")
    tp = lax.axis_index("tp")
    x = ep // 2
    k = ep - 2 * x
    return ep, tp, x, k


def _remote(src, dst, ssem, rsem, ep, tp):
    return pltpu.make_async_remote_copy(
        src_ref=src, dst_ref=dst, send_sem=ssem, recv_sem=rsem,
        device_id={"ep": ep, "tp": tp}, device_id_type=MESH)


def dispatch_kernel(nbuf, tok_ref, ids_ref, gates_ref, wg_hbm, wu_hbm, h_hbm, cidx_ref, gk_ref,
                    rb, ids_all, gates_all, x_ref, wg_buf, wu_buf, h_buf, rank_ref, rankg_ref,
                    wsem, hsem, xsend, ysend, ssend, trecv, srecv, msend, mrecv):
    experts, load = x_ref.shape[0], x_ref.shape[1]
    hidden = x_ref.shape[2]
    ff = wg_buf.shape[1]
    ep, tp, x, k = _coords()
    me = ep * 2 + tp
    sib = 2 * x + (1 - k)
    xn = 2 * (1 - x) + k
    yt = 1 - tp

    def weights(e, slot):
        return (pltpu.make_async_copy(wg_hbm.at[e], wg_buf.at[slot], wsem.at[0, slot]),
                pltpu.make_async_copy(wu_hbm.at[e], wu_buf.at[slot], wsem.at[1, slot]))

    for e in range(nbuf):
        for cp in weights(e, e):
            cp.start()

    others = []
    for step in range(1, NDEV):
        d = lax.rem(me + step, NDEV)
        others.append((d // 2, d % 2, step))
    barrier = pltpu.get_barrier_semaphore()
    for oe, ot, _ in others:
        pl.semaphore_signal(barrier, inc=1, device_id={"ep": oe, "tp": ot}, device_id_type=MESH)
    pl.semaphore_wait(barrier, NDEV - 1)

    metas = []
    for oe, ot, step in others:
        for which, (src, dst) in enumerate(((ids_ref, ids_all), (gates_ref, gates_all))):
            cp = _remote(src, dst.at[me], msend.at[which, step - 1], mrecv.at[which, step - 1], oe, ot)
            cp.start()
            metas.append(cp)

    rows = (pl.ds(0, HALF), pl.ds(HALF, HALF))
    wide = hidden // 2
    cols = (pl.ds(0, wide), pl.ds(wide, wide))
    xs, ys, sibs = {}, {}, {}
    for c in range(2):
        for g in (1, 2):
            part = rows[g - 1], rows[2 - g]
            xs[g, c] = _remote(tok_ref.at[part[0], cols[c]], rb.at[g, rows[0], cols[c]],
                               xsend.at[g - 1, c], trecv.at[g - 1, 0, c], xn, tp)
            ys[g, c] = _remote(tok_ref.at[part[1], cols[c]], rb.at[g, rows[1], cols[c]],
                               ysend.at[g - 1, c], trecv.at[g - 1, 1, c], ep, yt)
        ys[3, c] = _remote(rb.at[1, rows[0], cols[c]], rb.at[3, rows[0], cols[c]],
                           ysend.at[2, c], trecv.at[2, 0, c], ep, yt)
        xs[3, c] = _remote(rb.at[1, rows[1], cols[c]], rb.at[3, rows[1], cols[c]],
                           xsend.at[2, c], trecv.at[2, 1, c], xn, tp)
        for g in (1, 2, 3):
            sibs[g, c] = _remote(rb.at[g, :, cols[c]], rb.at[4 + g, :, cols[c]],
                                 ssend.at[g, c], srecv.at[g, c], sib, tp)
    sib_own = _remote(tok_ref, rb.at[4], ssend.at[0, 0], srecv.at[0, 0], sib, tp)
    for g in (1, 2):
        for c in range(2):
            xs[g, c].start()
            ys[g, c].start()
    sib_own.start()

    def arrived(g, c):
        xs[g, c].wait_recv()
        ys[g, c].wait_recv()
        if g == 1:
            ys[3, c].start()
            xs[3, c].start()
        sibs[g, c].start()

    ids_all[me] = ids_ref[...]
    gates_all[me] = gates_ref[...]
    for cp in metas:
        cp.wait_recv()
    row_i = lax.broadcasted_iota(jnp.int32, (ROWS, ROWS), 0)
    col_i = lax.broadcasted_iota(jnp.int32, (ROWS, ROWS), 1)
    before = jnp.where(row_i < col_i, 1.0, 0.0).astype(BF16)
    e_row = lax.broadcasted_iota(jnp.int32, (experts, ROWS), 0)
    lower = jnp.where(lax.broadcasted_iota(jnp.int32, (experts, experts), 1)
                      < lax.broadcasted_iota(jnp.int32, (experts, experts), 0), 1.0, 0.0).astype(BF16)
    e_global = e_row + ep * experts
    e_base = e_row.astype(F32) * float(load)
    base = jnp.zeros((experts, 1), F32)
    for b in range(NDEV):
        ind = jnp.zeros((experts, ROWS), F32)
        gate = jnp.zeros((experts, ROWS), F32)
        for j in range(6):
            hit = ids_all[b, j:j + 1, :] == e_global
            ind = jnp.where(hit, 1.0, ind)
            gate = jnp.where(hit, gates_all[b, j:j + 1, :], gate)
        ind16 = ind.astype(BF16)
        rank = _dot(ind16, before) + base
        base = base + jnp.sum(ind, axis=1, keepdims=True)
        pos = _dot(lower, ind16)
        rank_ref[b] = jnp.where(ind > 0.5, rank, -1.0)
        slot = e_base + rank
        for c in range(TOPC):
            sel = (ind > 0.5) & (pos == float(c))
            idx = jnp.sum(jnp.where(sel, slot, 0.0), axis=0, keepdims=True)
            idx = idx.astype(jnp.int32)
            gk = jnp.sum(jnp.where(sel, gate, 0.0), axis=0, keepdims=True)
            for q in range(ROWS // 128):
                at = (c * NDEV + b) * (ROWS // 128) + q
                cidx_ref[at:at + 1, :] = idx[:, q * 128:(q + 1) * 128]
                gk_ref[at:at + 1, :] = gk[:, q * 128:(q + 1) * 128]
    for s in range(2):
        kk = k if s == 0 else 1 - k
        b_own = (2 * x + kk) * 2 + tp
        b_x = (2 * (1 - x) + kk) * 2 + tp
        b_y = (2 * x + kk) * 2 + yt
        b_d = (2 * (1 - x) + kk) * 2 + yt
        rankg_ref[4 * s] = rank_ref[b_own]
        rankg_ref[4 * s + 1, :, 0:HALF] = rank_ref[b_x, :, 0:HALF]
        rankg_ref[4 * s + 1, :, HALF:ROWS] = rank_ref[b_y, :, HALF:ROWS]
        rankg_ref[4 * s + 2, :, 0:HALF] = rank_ref[b_x, :, HALF:ROWS]
        rankg_ref[4 * s + 2, :, HALF:ROWS] = rank_ref[b_y, :, 0:HALF]
        rankg_ref[4 * s + 3] = rank_ref[b_d]

    def one_hot(q, e):
        want = lax.broadcasted_iota(jnp.int32, (load, ROWS), 0).astype(F32)
        return jnp.where(want == rankg_ref[q, pl.ds(e, 1), :], 1.0, 0.0).astype(BF16)

    def gather(e, g, c):
        oh0, oh1 = one_hot(g, e), one_hot(4 + g, e)
        for n in range(c * wide, (c + 1) * wide, 512):
            at = pl.ds(n, 512)
            left = tok_ref[:, at] if g == 0 else rb[g, :, at]
            got = (_dot(oh0, left) + _dot(oh1, rb[4 + g, :, at])).astype(BF16)
            if g == 0:
                x_ref[e, :, at] = got
            else:
                x_ref[e, :, at] = x_ref[e, :, at] + got

    def gather_all(g, halves, hook_at=None, hook=None):
        def body(e, carry):
            if hook is not None:
                pl.when(e == hook_at)(hook)
            for c in halves:
                gather(e, g, c)
            return carry
        lax.fori_loop(0, experts, body, 0)

    sib_own.wait_recv()
    gather_all(0, (0, 1), 8, lambda: arrived(1, 0))
    arrived(1, 1)
    sibs[1, 0].wait_recv()
    gather_all(1, (0,))
    arrived(2, 0)
    sibs[1, 1].wait_recv()
    gather_all(1, (1,))
    sibs[2, 0].wait_recv()
    gather_all(2, (0,), 3, lambda: arrived(2, 1))
    sibs[2, 1].wait_recv()
    gather_all(2, (1,), 8, lambda: arrived(3, 0))
    sibs[3, 0].wait_recv()
    gather_all(3, (0,), 12, lambda: arrived(3, 1))
    sibs[3, 1].wait_recv()

    def expert(e, carry):
        slot = lax.rem(e, nbuf)
        gather(e, 3, 1)
        for cp in weights(e, slot):
            cp.wait()
        for n0, n1 in ((0, 256), (256, 512), (512, ff)):
            a = _dot_t(wg_buf[slot, n0:n1, :], x_ref[e])
            b = _dot_t(wu_buf[slot, n0:n1, :], x_ref[e])
            h_buf[e, :, n0:n1] = (a * jax.nn.sigmoid(a) * b).T.astype(BF16)
        pltpu.make_async_copy(h_buf.at[e], h_hbm.at[e], hsem.at[e]).start()

        @pl.when(e + nbuf < experts)
        def _():
            for cp in weights(e + nbuf, slot):
                cp.start()
        return carry

    lax.fori_loop(0, experts, expert, 0)
    for e in range(experts):
        pltpu.make_async_copy(h_buf.at[e], h_hbm.at[e], hsem.at[e]).wait()
    for cp in metas + list(xs.values()) + list(ys.values()) + list(sibs.values()) + [sib_own]:
        cp.wait_send()


def return_kernel(nbuf, h_hbm, wd_hbm, cidx_hbm, gk_hbm, out_ref,
                  cidx_ref, gk_ref, h_ref, wd_buf, o_ref, psib, pown, r0, r1, r2,
                  hsem, wsem, s0, v0, s1, v1, s2, v2):
    experts, load = h_ref.shape[0], h_ref.shape[1]
    ncol = wd_hbm.shape[2] // COLS
    ep, tp, x, k = _coords()
    sib = 2 * x + (1 - k)
    xn = 2 * (1 - x) + k
    yt = 1 - tp

    def weights(i, slot):
        c, e = i // experts, i % experts
        cols = pl.ds(pl.multiple_of(c * COLS, COLS), COLS)
        return pltpu.make_async_copy(wd_hbm.at[e, :, cols], wd_buf.at[slot], wsem.at[slot])

    ins = [pltpu.make_async_copy(h_hbm, h_ref, hsem.at[0]),
           pltpu.make_async_copy(cidx_hbm, cidx_ref, hsem.at[1]),
           pltpu.make_async_copy(gk_hbm, gk_ref, hsem.at[2])]
    weights(0, 0).start()
    for cp in ins:
        cp.start()
    for i in range(1, nbuf):
        weights(i, i).start()

    barrier = pltpu.get_barrier_semaphore()
    for oe, ot in ((sib, tp), (xn, tp), (ep, yt)):
        pl.semaphore_signal(barrier, inc=1, device_id={"ep": oe, "tp": ot}, device_id_type=MESH)
    pl.semaphore_wait(barrier, 3)
    for cp in ins:
        cp.wait()

    o_lin = o_ref.reshape(experts * load * 8, 128)

    def down(c):
        def body(e, carry):
            i = c * experts + e
            slot = lax.rem(i, nbuf)
            weights(i, slot).wait()
            for n in range(0, COLS, 256):
                o = _dot(h_ref[e], wd_buf[slot, :, n:n + 256])
                for j in range(2):
                    at = e * (load * 8) + (n // 128 + j)
                    o_lin[pl.ds(at, load, stride=8), :] = o[:, j * 128:(j + 1) * 128]

            @pl.when(i + nbuf < ncol * experts)
            def _():
                weights(i + nbuf, slot).start()
            return carry
        lax.fori_loop(0, experts, body, 0)

    unroll = 16

    def combine(dst, blk):
        def body(i, carry):
            for u in range(unroll):
                r = i * unroll + u
                v = None
                for c in range(TOPC):
                    t = (blk * ROWS + i * unroll) + (c * NDEV * ROWS + u)
                    term = o_ref[cidx_ref[t]] * gk_ref[t]
                    v = term if v is None else v + term
                dst[pl.ds(pl.multiple_of(r * 8, 8), 8), :] = v
            return carry
        lax.fori_loop(0, ROWS // unroll, body, 0)

    tile = 256

    def add_into(dst, src, rows):
        def body(i, carry):
            at = pl.ds(pl.multiple_of(i * tile, tile), tile)
            dst[at, :] = dst[at, :] + src[at, :]
            return carry
        lax.fori_loop(0, rows // tile, body, 0)

    lo, hi = pl.ds(0, HALF * 8), pl.ds(HALF * 8, HALF * 8)

    def block(g, kk):
        xd = x if g < 2 else 1 - x
        yd = tp if g % 2 == 0 else 1 - tp
        return (2 * xd + kk) * 2 + yd

    stage0 = {(c, g): _remote(psib.at[c, g], r0.at[c, g], s0.at[c, g], v0.at[c, g], sib, tp)
              for c in range(ncol) for g in range(4)}
    stage1 = {}
    stage2 = {}
    for c in range(ncol):
        for d in range(2):
            stage1[c, 0, d] = _remote(pown.at[c, 2 + d, lo], r1.at[c, 0, d], s1.at[c, 0, d], v1.at[c, 0, d], xn, tp)
            stage1[c, 1, d] = _remote(pown.at[c, 1 + 2 * d, hi], r1.at[c, 1, d], s1.at[c, 1, d], v1.at[c, 1, d], ep, yt)
        stage2[c, 0] = _remote(pown.at[c, 1, lo], r2.at[c, 0], s2.at[c, 0], v2.at[c, 0], ep, yt)
        stage2[c, 1] = _remote(pown.at[c, 2, hi], r2.at[c, 1], s2.at[c, 1], v2.at[c, 1], xn, tp)

    def merge(c, g):
        combine(pown.at[c, g], block(g, k))
        stage0[c, g].wait_recv()
        add_into(pown.at[c, g], r0.at[c, g], ROWS * 8)

    for c in range(ncol):
        down(c)
        for g in (3, 2):
            combine(psib.at[c, g], block(g, 1 - k))
            stage0[c, g].start()
        merge(c, 3)
        stage1[c, 0, 1].start()
        stage1[c, 1, 1].start()
        combine(psib.at[c, 1], block(1, 1 - k))
        stage0[c, 1].start()
        merge(c, 2)
        stage1[c, 0, 0].start()
        combine(psib.at[c, 0], block(0, 1 - k))
        stage0[c, 0].start()
        merge(c, 1)
        stage1[c, 1, 0].start()
        merge(c, 0)
    for c in range(ncol):
        stage1[c, 0, 1].wait_recv()
        add_into(pown.at[c, 1, lo], r1.at[c, 0, 1], HALF * 8)
        stage2[c, 0].start()
        stage1[c, 1, 1].wait_recv()
        add_into(pown.at[c, 2, hi], r1.at[c, 1, 1], HALF * 8)
        stage2[c, 1].start()
    for c in range(ncol):
        for half in range(2):
            stage1[c, half, 0].wait_recv()
            add_into(pown.at[c, 0, lo if half == 0 else hi], r1.at[c, half, 0], HALF * 8)
    for c in range(ncol):
        for half in range(2):
            stage2[c, half].wait_recv()

            def body(i, carry, c=c, half=half):
                row = half * HALF + i * 16
                for j in range(8):
                    parts = []
                    for q in range(2):
                        at = (i * 16 + q * 8) * 8 + j
                        parts.append(pown[c, 0, pl.ds(half * HALF * 8 + at, 8, stride=8), :]
                                     + r2[c, half, pl.ds(at, 8, stride=8), :])
                    val = jnp.concatenate(parts, axis=0).astype(BF16)
                    out_ref[pl.ds(pl.multiple_of(row, 16), 16), c * COLS + j * 128:c * COLS + (j + 1) * 128] = val
                return carry
            lax.fori_loop(0, HALF // 16, body, 0)
    for cp in list(stage0.values()) + list(stage1.values()) + list(stage2.values()):
        cp.wait_send()


def solution(mesh):
    row_spec = P(("dp", "ep", "tp"), None)

    def local_layer(tokens, expert_ids, gates, w_gate, w_up, w_down):
        experts, hidden, ff = w_gate.shape
        top_k = expert_ids.shape[1]
        load = ROWS * NDEV * top_k // (experts * 4)
        nbuf = 4
        vm = pl.BlockSpec(memory_space=pltpu.VMEM)
        hbm = pl.BlockSpec(memory_space=pl.ANY)
        h, cidx, gk = pl.pallas_call(
            functools.partial(dispatch_kernel, nbuf),
            out_shape=(jax.ShapeDtypeStruct((experts, load, ff), BF16),
                       jax.ShapeDtypeStruct((TOPC * ROWS * NDEV // 128, 128), jnp.int32),
                       jax.ShapeDtypeStruct((TOPC * ROWS * NDEV // 128, 128), F32)),
            in_specs=[vm, vm, vm, hbm, hbm],
            out_specs=(hbm, vm, vm),
            scratch_shapes=[
                pltpu.VMEM((8, ROWS, hidden), BF16),
                pltpu.VMEM((NDEV, top_k, ROWS), jnp.int32),
                pltpu.VMEM((NDEV, top_k, ROWS), F32),
                pltpu.VMEM((experts, load, hidden), BF16),
                pltpu.VMEM((nbuf, ff, hidden), BF16),
                pltpu.VMEM((nbuf, ff, hidden), BF16),
                pltpu.VMEM((experts, load, ff), BF16),
                pltpu.VMEM((NDEV, experts, ROWS), F32),
                pltpu.VMEM((8, experts, ROWS), F32),
                pltpu.SemaphoreType.DMA((2, nbuf)),
                pltpu.SemaphoreType.DMA((experts,)),
                pltpu.SemaphoreType.DMA((3, 2)),
                pltpu.SemaphoreType.DMA((3, 2)),
                pltpu.SemaphoreType.DMA((4, 2)),
                pltpu.SemaphoreType.DMA((3, 2, 2)),
                pltpu.SemaphoreType.DMA((4, 2)),
                pltpu.SemaphoreType.DMA((2, NDEV - 1)),
                pltpu.SemaphoreType.DMA((2, NDEV - 1)),
            ],
            compiler_params=pltpu.CompilerParams(collective_id=0, has_side_effects=True, vmem_limit_bytes=63 * 2**20),
            name="dispatch_up",
        )(tokens, expert_ids.T, gates.T, jnp.swapaxes(w_gate, 1, 2), jnp.swapaxes(w_up, 1, 2))

        nbuf2 = 6
        ncol = hidden // COLS
        return pl.pallas_call(
            functools.partial(return_kernel, nbuf2),
            out_shape=jax.ShapeDtypeStruct((ROWS, hidden), BF16),
            in_specs=[hbm, hbm, hbm, hbm],
            out_specs=vm,
            scratch_shapes=[
                pltpu.SMEM((TOPC * ROWS * NDEV,), jnp.int32),
                pltpu.SMEM((TOPC * ROWS * NDEV,), F32),
                pltpu.VMEM((experts, load, ff), BF16),
                pltpu.VMEM((nbuf2, ff, COLS), BF16),
                pltpu.VMEM((experts * load, 8, 128), F32),
                pltpu.VMEM((ncol, 4, ROWS * 8, 128), F32),
                pltpu.VMEM((ncol, 4, ROWS * 8, 128), F32),
                pltpu.VMEM((ncol, 4, ROWS * 8, 128), F32),
                pltpu.VMEM((ncol, 2, 2, HALF * 8, 128), F32),
                pltpu.VMEM((ncol, 2, HALF * 8, 128), F32),
                pltpu.SemaphoreType.DMA((3,)),
                pltpu.SemaphoreType.DMA((nbuf2,)),
                pltpu.SemaphoreType.DMA((ncol, 4)),
                pltpu.SemaphoreType.DMA((ncol, 4)),
                pltpu.SemaphoreType.DMA((ncol, 2, 2)),
                pltpu.SemaphoreType.DMA((ncol, 2, 2)),
                pltpu.SemaphoreType.DMA((ncol, 2)),
                pltpu.SemaphoreType.DMA((ncol, 2)),
            ],
            compiler_params=pltpu.CompilerParams(collective_id=1, has_side_effects=True, vmem_limit_bytes=63 * 2**20),
            name="down_return",
        )(h, w_down, cidx.reshape(-1), gk.reshape(-1))

    return jax.shard_map(local_layer, mesh=mesh, in_specs=(row_spec, row_spec, row_spec, P("ep", None, "tp"), P("ep", None, "tp"), P("ep", "tp", None)), out_specs=row_spec, check_vma=False)
```

```python
import functools

import jax
import jax.numpy as jnp
from jax import lax
from jax.experimental import pallas as pl
from jax.experimental.pallas import tpu as pltpu
from jax.sharding import PartitionSpec as P

MESH = pl.DeviceIdType.MESH
F32 = jnp.float32
BF16 = jnp.bfloat16

ROWS = 256
HALF = ROWS // 2
NDEV = 8
TOPC = 3
COLS = 1024


def _dot(a, b):
    return jnp.dot(a, b, preferred_element_type=F32)


def _dot_t(a, b):
    return lax.dot_general(a, b, (((1,), (1,)), ((), ())), preferred_element_type=F32)


def _coords():
    ep = lax.axis_index("ep")
    tp = lax.axis_index("tp")
    x = ep // 2
    k = ep - 2 * x
    return ep, tp, x, k


def _remote(src, dst, ssem, rsem, ep, tp):
    return pltpu.make_async_remote_copy(
        src_ref=src, dst_ref=dst, send_sem=ssem, recv_sem=rsem,
        device_id={"ep": ep, "tp": tp}, device_id_type=MESH)


def dispatch_kernel(nbuf, tok_ref, ids_ref, gates_ref, wg_hbm, wu_hbm, h_hbm, cidx_ref, gk_ref,
                    rb, ids_all, gates_all, x_ref, wg_buf, wu_buf, h_buf, rank_ref, rankg_ref,
                    wsem, hsem, xsend, ysend, ssend, trecv, srecv, msend, mrecv):
    experts, load = x_ref.shape[0], x_ref.shape[1]
    hidden = x_ref.shape[2]
    ff = wg_buf.shape[1]
    ep, tp, x, k = _coords()
    me = ep * 2 + tp
    sib = 2 * x + (1 - k)
    xn = 2 * (1 - x) + k
    yt = 1 - tp

    def weights(e, slot):
        return (pltpu.make_async_copy(wg_hbm.at[e], wg_buf.at[slot], wsem.at[0, slot]),
                pltpu.make_async_copy(wu_hbm.at[e], wu_buf.at[slot], wsem.at[1, slot]))

    for e in range(nbuf):
        for cp in weights(e, e):
            cp.start()

    others = []
    for step in range(1, NDEV):
        d = lax.rem(me + step, NDEV)
        others.append((d // 2, d % 2, step))
    barrier = pltpu.get_barrier_semaphore()
    for oe, ot, _ in others:
        pl.semaphore_signal(barrier, inc=1, device_id={"ep": oe, "tp": ot}, device_id_type=MESH)
    pl.semaphore_wait(barrier, NDEV - 1)

    metas = []
    for oe, ot, step in others:
        for which, (src, dst) in enumerate(((ids_ref, ids_all), (gates_ref, gates_all))):
            cp = _remote(src, dst.at[me], msend.at[which, step - 1], mrecv.at[which, step - 1], oe, ot)
            cp.start()
            metas.append(cp)

    rows = (pl.ds(0, HALF), pl.ds(HALF, HALF))
    wide = hidden // 2
    cols = (pl.ds(0, wide), pl.ds(wide, wide))
    xs, ys, sibs = {}, {}, {}
    for c in range(2):
        for g in (1, 2):
            part = rows[g - 1], rows[2 - g]
            xs[g, c] = _remote(tok_ref.at[part[0], cols[c]], rb.at[g, rows[0], cols[c]],
                               xsend.at[g - 1, c], trecv.at[g - 1, 0, c], xn, tp)
            ys[g, c] = _remote(tok_ref.at[part[1], cols[c]], rb.at[g, rows[1], cols[c]],
                               ysend.at[g - 1, c], trecv.at[g - 1, 1, c], ep, yt)
        ys[3, c] = _remote(rb.at[1, rows[0], cols[c]], rb.at[3, rows[0], cols[c]],
                           ysend.at[2, c], trecv.at[2, 0, c], ep, yt)
        xs[3, c] = _remote(rb.at[1, rows[1], cols[c]], rb.at[3, rows[1], cols[c]],
                           xsend.at[2, c], trecv.at[2, 1, c], xn, tp)
        for g in (1, 2, 3):
            sibs[g, c] = _remote(rb.at[g, :, cols[c]], rb.at[4 + g, :, cols[c]],
                                 ssend.at[g, c], srecv.at[g, c], sib, tp)
    sib_own = _remote(tok_ref, rb.at[4], ssend.at[0, 0], srecv.at[0, 0], sib, tp)
    for g in (1, 2):
        for c in range(2):
            xs[g, c].start()
            ys[g, c].start()
    sib_own.start()

    def arrived(g, c):
        xs[g, c].wait_recv()
        ys[g, c].wait_recv()
        if g == 1:
            ys[3, c].start()
            xs[3, c].start()
        sibs[g, c].start()

    ids_all[me] = ids_ref[...]
    gates_all[me] = gates_ref[...]
    for cp in metas:
        cp.wait_recv()
    row_i = lax.broadcasted_iota(jnp.int32, (ROWS, ROWS), 0)
    col_i = lax.broadcasted_iota(jnp.int32, (ROWS, ROWS), 1)
    before = jnp.where(row_i < col_i, 1.0, 0.0).astype(BF16)
    e_row = lax.broadcasted_iota(jnp.int32, (experts, ROWS), 0)
    lower = jnp.where(lax.broadcasted_iota(jnp.int32, (experts, experts), 1)
                      < lax.broadcasted_iota(jnp.int32, (experts, experts), 0), 1.0, 0.0).astype(BF16)
    e_global = e_row + ep * experts
    e_base = e_row.astype(F32) * float(load)
    base = jnp.zeros((experts, 1), F32)
    for b in range(NDEV):
        ind = jnp.zeros((experts, ROWS), F32)
        gate = jnp.zeros((experts, ROWS), F32)
        for j in range(6):
            hit = ids_all[b, j:j + 1, :] == e_global
            ind = jnp.where(hit, 1.0, ind)
            gate = jnp.where(hit, gates_all[b, j:j + 1, :], gate)
        ind16 = ind.astype(BF16)
        rank = _dot(ind16, before) + base
        base = base + jnp.sum(ind, axis=1, keepdims=True)
        pos = _dot(lower, ind16)
        rank_ref[b] = jnp.where(ind > 0.5, rank, -1.0)
        slot = e_base + rank
        for c in range(TOPC):
            sel = (ind > 0.5) & (pos == float(c))
            idx = jnp.sum(jnp.where(sel, slot, 0.0), axis=0, keepdims=True)
            idx = idx.astype(jnp.int32)
            gk = jnp.sum(jnp.where(sel, gate, 0.0), axis=0, keepdims=True)
            for q in range(ROWS // 128):
                at = (c * NDEV + b) * (ROWS // 128) + q
                cidx_ref[at:at + 1, :] = idx[:, q * 128:(q + 1) * 128]
                gk_ref[at:at + 1, :] = gk[:, q * 128:(q + 1) * 128]
    for s in range(2):
        kk = k if s == 0 else 1 - k
        b_own = (2 * x + kk) * 2 + tp
        b_x = (2 * (1 - x) + kk) * 2 + tp
        b_y = (2 * x + kk) * 2 + yt
        b_d = (2 * (1 - x) + kk) * 2 + yt
        rankg_ref[4 * s] = rank_ref[b_own]
        rankg_ref[4 * s + 1, :, 0:HALF] = rank_ref[b_x, :, 0:HALF]
        rankg_ref[4 * s + 1, :, HALF:ROWS] = rank_ref[b_y, :, HALF:ROWS]
        rankg_ref[4 * s + 2, :, 0:HALF] = rank_ref[b_x, :, HALF:ROWS]
        rankg_ref[4 * s + 2, :, HALF:ROWS] = rank_ref[b_y, :, 0:HALF]
        rankg_ref[4 * s + 3] = rank_ref[b_d]

    def one_hot(q, e):
        want = lax.broadcasted_iota(jnp.int32, (load, ROWS), 0).astype(F32)
        return jnp.where(want == rankg_ref[q, pl.ds(e, 1), :], 1.0, 0.0).astype(BF16)

    def gather(e, g, c):
        oh0, oh1 = one_hot(g, e), one_hot(4 + g, e)
        for n in range(c * wide, (c + 1) * wide, 512):
            at = pl.ds(n, 512)
            left = tok_ref[:, at] if g == 0 else rb[g, :, at]
            got = (_dot(oh0, left) + _dot(oh1, rb[4 + g, :, at])).astype(BF16)
            if g == 0:
                x_ref[e, :, at] = got
            else:
                x_ref[e, :, at] = x_ref[e, :, at] + got

    group = 4

    def gather_all(g, halves, hook_at=None, hook=None):
        def body(i, carry):
            if hook is not None:
                pl.when(i == hook_at)(hook)
            for u in range(group):
                for c in halves:
                    gather(i * group + u, g, c)
            return carry
        lax.fori_loop(0, experts // group, body, 0)

    sib_own.wait_recv()
    gather_all(0, (0, 1), 2, lambda: arrived(1, 0))
    arrived(1, 1)
    sibs[1, 0].wait_recv()
    gather_all(1, (0,))
    arrived(2, 0)
    sibs[1, 1].wait_recv()
    gather_all(1, (1,))
    sibs[2, 0].wait_recv()
    gather_all(2, (0,), 1, lambda: arrived(2, 1))
    sibs[2, 1].wait_recv()
    gather_all(2, (1,), 2, lambda: arrived(3, 0))
    sibs[3, 0].wait_recv()
    gather_all(3, (0,), 3, lambda: arrived(3, 1))
    sibs[3, 1].wait_recv()

    pair = 2

    def expert(i, carry):
        ids = [i * pair + u for u in range(pair)]
        for e in ids:
            for cp in weights(e, lax.rem(e, nbuf)):
                cp.wait()
        for e in ids:
            slot = lax.rem(e, nbuf)
            gather(e, 3, 1)
            for n0, n1 in ((0, 256), (256, 512), (512, ff)):
                a = _dot_t(wg_buf[slot, n0:n1, :], x_ref[e])
                b = _dot_t(wu_buf[slot, n0:n1, :], x_ref[e])
                h_buf[e, :, n0:n1] = (a * jax.nn.sigmoid(a) * b).T.astype(BF16)
        for e in ids:
            pltpu.make_async_copy(h_buf.at[e], h_hbm.at[e], hsem.at[e]).start()

        @pl.when(i * pair + nbuf < experts)
        def _():
            for e in ids:
                for cp in weights(e + nbuf, lax.rem(e, nbuf)):
                    cp.start()
        return carry

    lax.fori_loop(0, experts // pair, expert, 0)
    for e in range(experts):
        pltpu.make_async_copy(h_buf.at[e], h_hbm.at[e], hsem.at[e]).wait()
    for cp in metas + list(xs.values()) + list(ys.values()) + list(sibs.values()) + [sib_own]:
        cp.wait_send()


def return_kernel(nbuf, h_hbm, wd_hbm, cidx_hbm, gk_hbm, out_ref,
                  cidx_ref, gk_ref, h_ref, wd_buf, o_ref, psib, pown, r0, r1, r2,
                  hsem, wsem, s0, v0, s1, v1, s2, v2):
    experts, load = h_ref.shape[0], h_ref.shape[1]
    ncol = wd_hbm.shape[2] // COLS
    ep, tp, x, k = _coords()
    sib = 2 * x + (1 - k)
    xn = 2 * (1 - x) + k
    yt = 1 - tp

    def weights(i, slot):
        c, e = i // experts, i % experts
        cols = pl.ds(pl.multiple_of(c * COLS, COLS), COLS)
        return pltpu.make_async_copy(wd_hbm.at[e, :, cols], wd_buf.at[slot], wsem.at[slot])

    ins = [pltpu.make_async_copy(h_hbm, h_ref, hsem.at[0]),
           pltpu.make_async_copy(cidx_hbm, cidx_ref, hsem.at[1]),
           pltpu.make_async_copy(gk_hbm, gk_ref, hsem.at[2])]
    weights(0, 0).start()
    for cp in ins:
        cp.start()
    for i in range(1, nbuf):
        weights(i, i).start()

    barrier = pltpu.get_barrier_semaphore()
    for oe, ot in ((sib, tp), (xn, tp), (ep, yt)):
        pl.semaphore_signal(barrier, inc=1, device_id={"ep": oe, "tp": ot}, device_id_type=MESH)
    pl.semaphore_wait(barrier, 3)
    for cp in ins:
        cp.wait()

    o_lin = o_ref.reshape(experts * load * 8, 128)

    def down(c):
        def body(p, carry):
            ids = [p * 2 + u for u in range(2)]
            for e in ids:
                i = c * experts + e
                weights(i, lax.rem(i, nbuf)).wait()
            for e in ids:
                slot = lax.rem(c * experts + e, nbuf)
                for n in range(0, COLS, 256):
                    o = _dot(h_ref[e], wd_buf[slot, :, n:n + 256])
                    for j in range(2):
                        at = e * (load * 8) + (n // 128 + j)
                        o_lin[pl.ds(at, load, stride=8), :] = o[:, j * 128:(j + 1) * 128]

            @pl.when(c * experts + p * 2 + nbuf < ncol * experts)
            def _():
                for e in ids:
                    i = c * experts + e
                    weights(i + nbuf, lax.rem(i, nbuf)).start()
            return carry
        lax.fori_loop(0, experts // 2, body, 0)

    unroll = 16

    def combine(dst, blk):
        def body(i, carry):
            for u in range(unroll):
                r = i * unroll + u
                v = None
                for c in range(TOPC):
                    t = (blk * ROWS + i * unroll) + (c * NDEV * ROWS + u)
                    term = o_ref[cidx_ref[t]] * gk_ref[t]
                    v = term if v is None else v + term
                dst[pl.ds(pl.multiple_of(r * 8, 8), 8), :] = v
            return carry
        lax.fori_loop(0, ROWS // unroll, body, 0)

    tile = 256

    def add_into(dst, src, rows):
        def body(i, carry):
            at = pl.ds(pl.multiple_of(i * tile, tile), tile)
            dst[at, :] = dst[at, :] + src[at, :]
            return carry
        lax.fori_loop(0, rows // tile, body, 0)

    lo, hi = pl.ds(0, HALF * 8), pl.ds(HALF * 8, HALF * 8)

    def block(g, kk):
        xd = x if g < 2 else 1 - x
        yd = tp if g % 2 == 0 else 1 - tp
        return (2 * xd + kk) * 2 + yd

    stage0 = {(c, g): _remote(psib.at[c, g], r0.at[c, g], s0.at[c, g], v0.at[c, g], sib, tp)
              for c in range(ncol) for g in range(4)}
    stage1 = {}
    stage2 = {}
    for c in range(ncol):
        for d in range(2):
            stage1[c, 0, d] = _remote(pown.at[c, 2 + d, lo], r1.at[c, 0, d], s1.at[c, 0, d], v1.at[c, 0, d], xn, tp)
            stage1[c, 1, d] = _remote(pown.at[c, 1 + 2 * d, hi], r1.at[c, 1, d], s1.at[c, 1, d], v1.at[c, 1, d], ep, yt)
        stage2[c, 0] = _remote(pown.at[c, 1, lo], r2.at[c, 0], s2.at[c, 0], v2.at[c, 0], ep, yt)
        stage2[c, 1] = _remote(pown.at[c, 2, hi], r2.at[c, 1], s2.at[c, 1], v2.at[c, 1], xn, tp)

    def merge(c, g):
        combine(pown.at[c, g], block(g, k))
        stage0[c, g].wait_recv()
        add_into(pown.at[c, g], r0.at[c, g], ROWS * 8)

    for c in range(ncol):
        down(c)
        for g in (3, 2):
            combine(psib.at[c, g], block(g, 1 - k))
            stage0[c, g].start()
        merge(c, 3)
        stage1[c, 0, 1].start()
        stage1[c, 1, 1].start()
        combine(psib.at[c, 1], block(1, 1 - k))
        stage0[c, 1].start()
        merge(c, 2)
        stage1[c, 0, 0].start()
        combine(psib.at[c, 0], block(0, 1 - k))
        stage0[c, 0].start()
        merge(c, 1)
        stage1[c, 1, 0].start()
        merge(c, 0)
    for c in range(ncol):
        stage1[c, 0, 1].wait_recv()
        add_into(pown.at[c, 1, lo], r1.at[c, 0, 1], HALF * 8)
        stage2[c, 0].start()
        stage1[c, 1, 1].wait_recv()
        add_into(pown.at[c, 2, hi], r1.at[c, 1, 1], HALF * 8)
        stage2[c, 1].start()
    for c in range(ncol):
        for half in range(2):
            stage1[c, half, 0].wait_recv()
            add_into(pown.at[c, 0, lo if half == 0 else hi], r1.at[c, half, 0], HALF * 8)
    for c in range(ncol):
        for half in range(2):
            stage2[c, half].wait_recv()

            def body(i, carry, c=c, half=half):
                row = half * HALF + i * 16
                for j in range(8):
                    parts = []
                    for q in range(2):
                        at = (i * 16 + q * 8) * 8 + j
                        parts.append(pown[c, 0, pl.ds(half * HALF * 8 + at, 8, stride=8), :]
                                     + r2[c, half, pl.ds(at, 8, stride=8), :])
                    val = jnp.concatenate(parts, axis=0).astype(BF16)
                    out_ref[pl.ds(pl.multiple_of(row, 16), 16), c * COLS + j * 128:c * COLS + (j + 1) * 128] = val
                return carry
            lax.fori_loop(0, HALF // 16, body, 0)
    for cp in list(stage0.values()) + list(stage1.values()) + list(stage2.values()):
        cp.wait_send()


def solution(mesh):
    row_spec = P(("dp", "ep", "tp"), None)

    def local_layer(tokens, expert_ids, gates, w_gate, w_up, w_down):
        experts, hidden, ff = w_gate.shape
        top_k = expert_ids.shape[1]
        load = ROWS * NDEV * top_k // (experts * 4)
        nbuf = 6
        vm = pl.BlockSpec(memory_space=pltpu.VMEM)
        hbm = pl.BlockSpec(memory_space=pl.ANY)
        h, cidx, gk = pl.pallas_call(
            functools.partial(dispatch_kernel, nbuf),
            out_shape=(jax.ShapeDtypeStruct((experts, load, ff), BF16),
                       jax.ShapeDtypeStruct((TOPC * ROWS * NDEV // 128, 128), jnp.int32),
                       jax.ShapeDtypeStruct((TOPC * ROWS * NDEV // 128, 128), F32)),
            in_specs=[vm, vm, vm, hbm, hbm],
            out_specs=(hbm, vm, vm),
            scratch_shapes=[
                pltpu.VMEM((8, ROWS, hidden), BF16),
                pltpu.VMEM((NDEV, top_k, ROWS), jnp.int32),
                pltpu.VMEM((NDEV, top_k, ROWS), F32),
                pltpu.VMEM((experts, load, hidden), BF16),
                pltpu.VMEM((nbuf, ff, hidden), BF16),
                pltpu.VMEM((nbuf, ff, hidden), BF16),
                pltpu.VMEM((experts, load, ff), BF16),
                pltpu.VMEM((NDEV, experts, ROWS), F32),
                pltpu.VMEM((8, experts, ROWS), F32),
                pltpu.SemaphoreType.DMA((2, nbuf)),
                pltpu.SemaphoreType.DMA((experts,)),
                pltpu.SemaphoreType.DMA((3, 2)),
                pltpu.SemaphoreType.DMA((3, 2)),
                pltpu.SemaphoreType.DMA((4, 2)),
                pltpu.SemaphoreType.DMA((3, 2, 2)),
                pltpu.SemaphoreType.DMA((4, 2)),
                pltpu.SemaphoreType.DMA((2, NDEV - 1)),
                pltpu.SemaphoreType.DMA((2, NDEV - 1)),
            ],
            compiler_params=pltpu.CompilerParams(collective_id=0, has_side_effects=True, vmem_limit_bytes=63 * 2**20),
            name="dispatch_up",
        )(tokens, expert_ids.T, gates.T, jnp.swapaxes(w_gate, 1, 2), jnp.swapaxes(w_up, 1, 2))

        nbuf2 = 8
        ncol = hidden // COLS
        return pl.pallas_call(
            functools.partial(return_kernel, nbuf2),
            out_shape=jax.ShapeDtypeStruct((ROWS, hidden), BF16),
            in_specs=[hbm, hbm, hbm, hbm],
            out_specs=vm,
            scratch_shapes=[
                pltpu.SMEM((TOPC * ROWS * NDEV,), jnp.int32),
                pltpu.SMEM((TOPC * ROWS * NDEV,), F32),
                pltpu.VMEM((experts, load, ff), BF16),
                pltpu.VMEM((nbuf2, ff, COLS), BF16),
                pltpu.VMEM((experts * load, 8, 128), F32),
                pltpu.VMEM((ncol, 4, ROWS * 8, 128), F32),
                pltpu.VMEM((ncol, 4, ROWS * 8, 128), F32),
                pltpu.VMEM((ncol, 4, ROWS * 8, 128), F32),
                pltpu.VMEM((ncol, 2, 2, HALF * 8, 128), F32),
                pltpu.VMEM((ncol, 2, HALF * 8, 128), F32),
                pltpu.SemaphoreType.DMA((3,)),
                pltpu.SemaphoreType.DMA((nbuf2,)),
                pltpu.SemaphoreType.DMA((ncol, 4)),
                pltpu.SemaphoreType.DMA((ncol, 4)),
                pltpu.SemaphoreType.DMA((ncol, 2, 2)),
                pltpu.SemaphoreType.DMA((ncol, 2, 2)),
                pltpu.SemaphoreType.DMA((ncol, 2)),
                pltpu.SemaphoreType.DMA((ncol, 2)),
            ],
            compiler_params=pltpu.CompilerParams(collective_id=1, has_side_effects=True, vmem_limit_bytes=63 * 2**20),
            name="down_return",
        )(h, w_down, cidx.reshape(-1), gk.reshape(-1))

    return jax.shard_map(local_layer, mesh=mesh, in_specs=(row_spec, row_spec, row_spec, P("ep", None, "tp"), P("ep", None, "tp"), P("ep", "tp", None)), out_specs=row_spec, check_vma=False)
```

```python
import functools

import jax
import jax.numpy as jnp
from jax import lax
from jax.experimental import pallas as pl
from jax.experimental.pallas import tpu as pltpu
from jax.sharding import PartitionSpec as P

MESH = pl.DeviceIdType.MESH
F32 = jnp.float32
BF16 = jnp.bfloat16

ROWS = 256
HALF = ROWS // 2
NDEV = 8
TOPC = 3
COLS = 1024


def _dot(a, b):
    return jnp.dot(a, b, preferred_element_type=F32)


def _dot_t(a, b):
    return lax.dot_general(a, b, (((1,), (1,)), ((), ())), preferred_element_type=F32)


def _coords():
    ep = lax.axis_index("ep")
    tp = lax.axis_index("tp")
    x = ep // 2
    k = ep - 2 * x
    return ep, tp, x, k


def _remote(src, dst, ssem, rsem, ep, tp):
    return pltpu.make_async_remote_copy(
        src_ref=src, dst_ref=dst, send_sem=ssem, recv_sem=rsem,
        device_id={"ep": ep, "tp": tp}, device_id_type=MESH)


def dispatch_kernel(nbuf, tok_ref, ids_ref, gates_ref, wg_hbm, wu_hbm, h_hbm, cidx_ref, gk_ref,
                    rb, ids_all, gates_all, x_ref, wg_buf, wu_buf, part_ref, h_buf, rank_ref, rankg_ref,
                    wsem, hsem, xsend, ysend, ssend, trecv, srecv, msend, mrecv):
    experts, load = x_ref.shape[0], x_ref.shape[1]
    hidden = x_ref.shape[2]
    ff = wg_buf.shape[1]
    ep, tp, x, k = _coords()
    me = ep * 2 + tp
    sib = 2 * x + (1 - k)
    xn = 2 * (1 - x) + k
    yt = 1 - tp

    wide = hidden // 2

    def weights(i, slot):
        e, at = i % experts, pl.ds(pl.multiple_of(i // experts * wide, wide), wide)
        return (pltpu.make_async_copy(wg_hbm.at[e, :, at], wg_buf.at[slot], wsem.at[0, slot]),
                pltpu.make_async_copy(wu_hbm.at[e, :, at], wu_buf.at[slot], wsem.at[1, slot]))

    for i in range(nbuf):
        for cp in weights(i, i):
            cp.start()

    others = []
    for step in range(1, NDEV):
        d = lax.rem(me + step, NDEV)
        others.append((d // 2, d % 2, step))
    barrier = pltpu.get_barrier_semaphore()
    for oe, ot, _ in others:
        pl.semaphore_signal(barrier, inc=1, device_id={"ep": oe, "tp": ot}, device_id_type=MESH)
    pl.semaphore_wait(barrier, NDEV - 1)

    metas = []
    for oe, ot, step in others:
        for which, (src, dst) in enumerate(((ids_ref, ids_all), (gates_ref, gates_all))):
            cp = _remote(src, dst.at[me], msend.at[which, step - 1], mrecv.at[which, step - 1], oe, ot)
            cp.start()
            metas.append(cp)

    rows = (pl.ds(0, HALF), pl.ds(HALF, HALF))
    cols = (pl.ds(0, wide), pl.ds(wide, wide))
    xs, ys, sibs = {}, {}, {}
    for c in range(2):
        for g in (1, 2):
            part = rows[g - 1], rows[2 - g]
            xs[g, c] = _remote(tok_ref.at[part[0], cols[c]], rb.at[g, rows[0], cols[c]],
                               xsend.at[g - 1, c], trecv.at[g - 1, 0, c], xn, tp)
            ys[g, c] = _remote(tok_ref.at[part[1], cols[c]], rb.at[g, rows[1], cols[c]],
                               ysend.at[g - 1, c], trecv.at[g - 1, 1, c], ep, yt)
        ys[3, c] = _remote(rb.at[1, rows[0], cols[c]], rb.at[3, rows[0], cols[c]],
                           ysend.at[2, c], trecv.at[2, 0, c], ep, yt)
        xs[3, c] = _remote(rb.at[1, rows[1], cols[c]], rb.at[3, rows[1], cols[c]],
                           xsend.at[2, c], trecv.at[2, 1, c], xn, tp)
        for g in (1, 2, 3):
            sibs[g, c] = _remote(rb.at[g, :, cols[c]], rb.at[4 + g, :, cols[c]],
                                 ssend.at[g, c], srecv.at[g, c], sib, tp)
    sib_own = _remote(tok_ref, rb.at[4], ssend.at[0, 0], srecv.at[0, 0], sib, tp)
    for g in (1, 2):
        xs[g, 0].start()
        ys[g, 0].start()
    sib_own.start()

    def arrived(g, c):
        xs[g, c].wait_recv()
        ys[g, c].wait_recv()
        if g == 1:
            ys[3, c].start()
            xs[3, c].start()
        sibs[g, c].start()
        if (g, c) == (1, 0):
            for q in (1, 2):
                xs[q, 1].start()
                ys[q, 1].start()

    ids_all[me] = ids_ref[...]
    gates_all[me] = gates_ref[...]
    for cp in metas:
        cp.wait_recv()
    row_i = lax.broadcasted_iota(jnp.int32, (ROWS, ROWS), 0)
    col_i = lax.broadcasted_iota(jnp.int32, (ROWS, ROWS), 1)
    before = jnp.where(row_i < col_i, 1.0, 0.0).astype(BF16)
    e_row = lax.broadcasted_iota(jnp.int32, (experts, ROWS), 0)
    lower = jnp.where(lax.broadcasted_iota(jnp.int32, (experts, experts), 1)
                      < lax.broadcasted_iota(jnp.int32, (experts, experts), 0), 1.0, 0.0).astype(BF16)
    e_global = e_row + ep * experts
    e_base = e_row.astype(F32) * float(load)
    base = jnp.zeros((experts, 1), F32)
    for b in range(NDEV):
        ind = jnp.zeros((experts, ROWS), F32)
        gate = jnp.zeros((experts, ROWS), F32)
        for j in range(6):
            hit = ids_all[b, j:j + 1, :] == e_global
            ind = jnp.where(hit, 1.0, ind)
            gate = jnp.where(hit, gates_all[b, j:j + 1, :], gate)
        ind16 = ind.astype(BF16)
        rank = _dot(ind16, before) + base
        base = base + jnp.sum(ind, axis=1, keepdims=True)
        pos = _dot(lower, ind16)
        rank_ref[b] = jnp.where(ind > 0.5, rank, -1.0)
        slot = e_base + rank
        for c in range(TOPC):
            sel = (ind > 0.5) & (pos == float(c))
            idx = jnp.sum(jnp.where(sel, slot, 0.0), axis=0, keepdims=True)
            idx = idx.astype(jnp.int32)
            gk = jnp.sum(jnp.where(sel, gate, 0.0), axis=0, keepdims=True)
            for q in range(ROWS // 128):
                at = (c * NDEV + b) * (ROWS // 128) + q
                cidx_ref[at:at + 1, :] = idx[:, q * 128:(q + 1) * 128]
                gk_ref[at:at + 1, :] = gk[:, q * 128:(q + 1) * 128]
    for s in range(2):
        kk = k if s == 0 else 1 - k
        b_own = (2 * x + kk) * 2 + tp
        b_x = (2 * (1 - x) + kk) * 2 + tp
        b_y = (2 * x + kk) * 2 + yt
        b_d = (2 * (1 - x) + kk) * 2 + yt
        rankg_ref[4 * s] = rank_ref[b_own]
        rankg_ref[4 * s + 1, :, 0:HALF] = rank_ref[b_x, :, 0:HALF]
        rankg_ref[4 * s + 1, :, HALF:ROWS] = rank_ref[b_y, :, HALF:ROWS]
        rankg_ref[4 * s + 2, :, 0:HALF] = rank_ref[b_x, :, HALF:ROWS]
        rankg_ref[4 * s + 2, :, HALF:ROWS] = rank_ref[b_y, :, 0:HALF]
        rankg_ref[4 * s + 3] = rank_ref[b_d]

    def one_hot(q, e):
        want = lax.broadcasted_iota(jnp.int32, (load, ROWS), 0).astype(F32)
        return jnp.where(want == rankg_ref[q, pl.ds(e, 1), :], 1.0, 0.0).astype(BF16)

    def gather(e, g, c):
        oh0, oh1 = one_hot(g, e), one_hot(4 + g, e)
        for n in range(c * wide, (c + 1) * wide, 512):
            at = pl.ds(n, 512)
            left = tok_ref[:, at] if g == 0 else rb[g, :, at]
            got = (_dot(oh0, left) + _dot(oh1, rb[4 + g, :, at])).astype(BF16)
            if g == 0:
                x_ref[e, :, at] = got
            else:
                x_ref[e, :, at] = x_ref[e, :, at] + got

    group = 4

    def gather_all(g, halves, hook_at=None, hook=None):
        def body(i, carry):
            if hook is not None:
                pl.when(i == hook_at)(hook)
            for u in range(group):
                for c in halves:
                    gather(i * group + u, g, c)
            return carry
        lax.fori_loop(0, experts // group, body, 0)

    sib_own.wait_recv()
    gather_all(0, (0, 1), 2, lambda: arrived(1, 0))
    sibs[1, 0].wait_recv()
    gather_all(1, (0,), 2, lambda: arrived(2, 0))
    sibs[2, 0].wait_recv()
    gather_all(2, (0,), 3, lambda: arrived(3, 0))
    sibs[3, 0].wait_recv()
    gather_all(3, (0,))
    arrived(1, 1)

    pair = 2

    def up_pass(c, hooks):
        def body(j, carry):
            for at, hook in hooks:
                pl.when(j == at)(hook)
            ids = [j * pair + u for u in range(pair)]
            slots = [lax.rem(c * experts + e, nbuf) for e in ids]
            for e, slot in zip(ids, slots):
                for cp in weights(c * experts + e, slot):
                    cp.wait()
            if c == 1:
                @pl.when(j * pair >= hslots)
                def _():
                    for e in ids:
                        h_out(e - hslots).wait()
            for e, slot in zip(ids, slots):
                for n0, n1 in ((0, 256), (256, 512), (512, ff)):
                    xe = x_ref[e, :, cols[c]]
                    a = _dot_t(wg_buf[slot, n0:n1, :], xe)
                    b = _dot_t(wu_buf[slot, n0:n1, :], xe)
                    if c == 0:
                        part_ref[0, e, n0:n1, :] = a
                        part_ref[1, e, n0:n1, :] = b
                    else:
                        a = part_ref[0, e, n0:n1, :] + a
                        b = part_ref[1, e, n0:n1, :] + b
                        h_buf[lax.rem(e, hslots), :, n0:n1] = (a * jax.nn.sigmoid(a) * b).astype(BF16).T
            if c == 1:
                for e in ids:
                    h_out(e).start()

            @pl.when(c * experts + j * pair + nbuf < 2 * experts)
            def _():
                for e, slot in zip(ids, slots):
                    for cp in weights(c * experts + e + nbuf, slot):
                        cp.start()
            return carry
        lax.fori_loop(0, experts // pair, body, 0)

    hslots = h_buf.shape[0]

    def h_out(e):
        slot = lax.rem(e, hslots)
        return pltpu.make_async_copy(h_buf.at[slot], h_hbm.at[e], hsem.at[slot])

    up_pass(0, ((3, lambda: arrived(2, 1)), (6, lambda: arrived(3, 1))))
    for g in (1, 2, 3):
        sibs[g, 1].wait_recv()
        gather_all(g, (1,))
    up_pass(1, ())
    for e in range(experts - hslots, experts):
        h_out(e).wait()
    for cp in metas + list(xs.values()) + list(ys.values()) + list(sibs.values()) + [sib_own]:
        cp.wait_send()


def return_kernel(nbuf, h_hbm, wd_hbm, cidx_hbm, gk_hbm, out_ref,
                  cidx_ref, gk_ref, h_ref, wd_buf, o_ref, psib, pown, r0, r1, r2,
                  hsem, wsem, s0, v0, s1, v1, s2, v2):
    experts, load = h_ref.shape[0], h_ref.shape[1]
    ncol = wd_hbm.shape[2] // COLS
    ep, tp, x, k = _coords()
    sib = 2 * x + (1 - k)
    xn = 2 * (1 - x) + k
    yt = 1 - tp

    def weights(i, slot):
        c, e = i // experts, i % experts
        cols = pl.ds(pl.multiple_of(c * COLS, COLS), COLS)
        return pltpu.make_async_copy(wd_hbm.at[e, :, cols], wd_buf.at[slot], wsem.at[slot])

    ins = [pltpu.make_async_copy(h_hbm, h_ref, hsem.at[0]),
           pltpu.make_async_copy(cidx_hbm, cidx_ref, hsem.at[1]),
           pltpu.make_async_copy(gk_hbm, gk_ref, hsem.at[2])]
    weights(0, 0).start()
    for cp in ins:
        cp.start()
    for i in range(1, nbuf):
        weights(i, i).start()

    barrier = pltpu.get_barrier_semaphore()
    for oe, ot in ((sib, tp), (xn, tp), (ep, yt)):
        pl.semaphore_signal(barrier, inc=1, device_id={"ep": oe, "tp": ot}, device_id_type=MESH)
    pl.semaphore_wait(barrier, 3)
    for cp in ins:
        cp.wait()

    o_lin = o_ref.reshape(experts * load * 8, 128)

    def down(c):
        def body(p, carry):
            ids = [p * 2 + u for u in range(2)]
            for e in ids:
                i = c * experts + e
                weights(i, lax.rem(i, nbuf)).wait()
            for e in ids:
                slot = lax.rem(c * experts + e, nbuf)
                for n in range(0, COLS, 256):
                    o = _dot(h_ref[e], wd_buf[slot, :, n:n + 256])
                    for j in range(2):
                        at = e * (load * 8) + (n // 128 + j)
                        o_lin[pl.ds(at, load, stride=8), :] = o[:, j * 128:(j + 1) * 128]

            @pl.when(c * experts + p * 2 + nbuf < ncol * experts)
            def _():
                for e in ids:
                    i = c * experts + e
                    weights(i + nbuf, lax.rem(i, nbuf)).start()
            return carry
        lax.fori_loop(0, experts // 2, body, 0)

    unroll = 16

    def combine(dst, blk, first=0, count=ROWS):
        def body(i, carry):
            for u in range(unroll):
                r = i * unroll + u
                v = None
                for c in range(TOPC):
                    t = (blk * ROWS + i * unroll) + (c * NDEV * ROWS + u)
                    term = o_ref[cidx_ref[t]] * gk_ref[t]
                    v = term if v is None else v + term
                dst[pl.ds(pl.multiple_of(r * 8, 8), 8), :] = v
            return carry
        lax.fori_loop(first // unroll, (first + count) // unroll, body, 0)

    tile = 256

    def add_into(dst, src, rows):
        def body(i, carry):
            at = pl.ds(pl.multiple_of(i * tile, tile), tile)
            dst[at, :] = dst[at, :] + src[at, :]
            return carry
        lax.fori_loop(0, rows // tile, body, 0)

    lo, hi = pl.ds(0, HALF * 8), pl.ds(HALF * 8, HALF * 8)

    def block(g, kk):
        xd = x if g < 2 else 1 - x
        yd = tp if g % 2 == 0 else 1 - tp
        return (2 * xd + kk) * 2 + yd

    halves = (lo, hi)
    stage0 = {(c, g): _remote(psib.at[c, g], r0.at[c, g], s0.at[c, g], v0.at[c, g], sib, tp)
              for c in range(ncol) for g in range(3)}
    for c in range(ncol):
        for half in range(2):
            at = halves[half]
            stage0[c, 3, half] = _remote(psib.at[c, 3, at], r0.at[c, 3, at], s0.at[c, 3 + half], v0.at[c, 3 + half], sib, tp)
    stage1 = {}
    stage2 = {}
    for c in range(ncol):
        for d in range(2):
            stage1[c, 0, d] = _remote(pown.at[c, 2 + d, lo], r1.at[c, 0, d], s1.at[c, 0, d], v1.at[c, 0, d], xn, tp)
            stage1[c, 1, d] = _remote(pown.at[c, 1 + 2 * d, hi], r1.at[c, 1, d], s1.at[c, 1, d], v1.at[c, 1, d], ep, yt)
        stage2[c, 0] = _remote(pown.at[c, 1, lo], r2.at[c, 0], s2.at[c, 0], v2.at[c, 0], ep, yt)
        stage2[c, 1] = _remote(pown.at[c, 2, hi], r2.at[c, 1], s2.at[c, 1], v2.at[c, 1], xn, tp)

    def merge(c, g):
        combine(pown.at[c, g], block(g, k))
        stage0[c, g].wait_recv()
        add_into(pown.at[c, g], r0.at[c, g], ROWS * 8)

    for c in range(ncol):
        down(c)
        for half in range(2):
            combine(psib.at[c, 3], block(3, 1 - k), half * HALF, HALF)
            stage0[c, 3, half].start()
        for half in range(2):
            combine(pown.at[c, 3], block(3, k), half * HALF, HALF)
            stage0[c, 3, half].wait_recv()
            add_into(pown.at[c, 3, halves[half]], r0.at[c, 3, halves[half]], HALF * 8)
            stage1[c, half, 1].start()
        combine(psib.at[c, 2], block(2, 1 - k))
        stage0[c, 2].start()
        combine(psib.at[c, 1], block(1, 1 - k))
        stage0[c, 1].start()
        merge(c, 2)
        stage1[c, 0, 0].start()
        combine(psib.at[c, 0], block(0, 1 - k))
        stage0[c, 0].start()
        merge(c, 1)
        stage1[c, 1, 0].start()
        merge(c, 0)
    for c in range(ncol):
        stage1[c, 0, 1].wait_recv()
        add_into(pown.at[c, 1, lo], r1.at[c, 0, 1], HALF * 8)
        stage2[c, 0].start()
        stage1[c, 1, 1].wait_recv()
        add_into(pown.at[c, 2, hi], r1.at[c, 1, 1], HALF * 8)
        stage2[c, 1].start()
    for c in range(ncol):
        for half in range(2):
            stage1[c, half, 0].wait_recv()
            add_into(pown.at[c, 0, lo if half == 0 else hi], r1.at[c, half, 0], HALF * 8)
    for c in range(ncol):
        for half in range(2):
            stage2[c, half].wait_recv()

            def body(i, carry, c=c, half=half):
                row = half * HALF + i * 16
                for j in range(8):
                    parts = []
                    for q in range(2):
                        at = (i * 16 + q * 8) * 8 + j
                        parts.append(pown[c, 0, pl.ds(half * HALF * 8 + at, 8, stride=8), :]
                                     + r2[c, half, pl.ds(at, 8, stride=8), :])
                    val = jnp.concatenate(parts, axis=0).astype(BF16)
                    out_ref[pl.ds(pl.multiple_of(row, 16), 16), c * COLS + j * 128:c * COLS + (j + 1) * 128] = val
                return carry
            lax.fori_loop(0, HALF // 16, body, 0)
    for cp in list(stage0.values()) + list(stage1.values()) + list(stage2.values()):
        cp.wait_send()


def solution(mesh):
    row_spec = P(("dp", "ep", "tp"), None)

    def local_layer(tokens, expert_ids, gates, w_gate, w_up, w_down):
        experts, hidden, ff = w_gate.shape
        top_k = expert_ids.shape[1]
        load = ROWS * NDEV * top_k // (experts * 4)
        nbuf = 6
        vm = pl.BlockSpec(memory_space=pltpu.VMEM)
        hbm = pl.BlockSpec(memory_space=pl.ANY)
        h, cidx, gk = pl.pallas_call(
            functools.partial(dispatch_kernel, nbuf),
            out_shape=(jax.ShapeDtypeStruct((experts, load, ff), BF16),
                       jax.ShapeDtypeStruct((TOPC * ROWS * NDEV // 128, 128), jnp.int32),
                       jax.ShapeDtypeStruct((TOPC * ROWS * NDEV // 128, 128), F32)),
            in_specs=[vm, vm, vm, hbm, hbm],
            out_specs=(hbm, vm, vm),
            scratch_shapes=[
                pltpu.VMEM((8, ROWS, hidden), BF16),
                pltpu.VMEM((NDEV, top_k, ROWS), jnp.int32),
                pltpu.VMEM((NDEV, top_k, ROWS), F32),
                pltpu.VMEM((experts, load, hidden), BF16),
                pltpu.VMEM((nbuf, ff, hidden // 2), BF16),
                pltpu.VMEM((nbuf, ff, hidden // 2), BF16),
                pltpu.VMEM((2, experts, ff, load), F32),
                pltpu.VMEM((4, load, ff), BF16),
                pltpu.VMEM((NDEV, experts, ROWS), F32),
                pltpu.VMEM((8, experts, ROWS), F32),
                pltpu.SemaphoreType.DMA((2, nbuf)),
                pltpu.SemaphoreType.DMA((4,)),
                pltpu.SemaphoreType.DMA((3, 2)),
                pltpu.SemaphoreType.DMA((3, 2)),
                pltpu.SemaphoreType.DMA((4, 2)),
                pltpu.SemaphoreType.DMA((3, 2, 2)),
                pltpu.SemaphoreType.DMA((4, 2)),
                pltpu.SemaphoreType.DMA((2, NDEV - 1)),
                pltpu.SemaphoreType.DMA((2, NDEV - 1)),
            ],
            compiler_params=pltpu.CompilerParams(collective_id=0, has_side_effects=True, vmem_limit_bytes=63 * 2**20),
            name="dispatch_up",
        )(tokens, expert_ids.T, gates.T, jnp.swapaxes(w_gate, 1, 2), jnp.swapaxes(w_up, 1, 2))

        nbuf2 = 8
        ncol = hidden // COLS
        return pl.pallas_call(
            functools.partial(return_kernel, nbuf2),
            out_shape=jax.ShapeDtypeStruct((ROWS, hidden), BF16),
            in_specs=[hbm, hbm, hbm, hbm],
            out_specs=vm,
            scratch_shapes=[
                pltpu.SMEM((TOPC * ROWS * NDEV,), jnp.int32),
                pltpu.SMEM((TOPC * ROWS * NDEV,), F32),
                pltpu.VMEM((experts, load, ff), BF16),
                pltpu.VMEM((nbuf2, ff, COLS), BF16),
                pltpu.VMEM((experts * load, 8, 128), F32),
                pltpu.VMEM((ncol, 4, ROWS * 8, 128), F32),
                pltpu.VMEM((ncol, 4, ROWS * 8, 128), F32),
                pltpu.VMEM((ncol, 4, ROWS * 8, 128), F32),
                pltpu.VMEM((ncol, 2, 2, HALF * 8, 128), F32),
                pltpu.VMEM((ncol, 2, HALF * 8, 128), F32),
                pltpu.SemaphoreType.DMA((3,)),
                pltpu.SemaphoreType.DMA((nbuf2,)),
                pltpu.SemaphoreType.DMA((ncol, 5)),
                pltpu.SemaphoreType.DMA((ncol, 5)),
                pltpu.SemaphoreType.DMA((ncol, 2, 2)),
                pltpu.SemaphoreType.DMA((ncol, 2, 2)),
                pltpu.SemaphoreType.DMA((ncol, 2)),
                pltpu.SemaphoreType.DMA((ncol, 2)),
            ],
            compiler_params=pltpu.CompilerParams(collective_id=1, has_side_effects=True, vmem_limit_bytes=63 * 2**20),
            name="down_return",
        )(h, w_down, cidx.reshape(-1), gk.reshape(-1))

    return jax.shard_map(local_layer, mesh=mesh, in_specs=(row_spec, row_spec, row_spec, P("ep", None, "tp"), P("ep", None, "tp"), P("ep", "tp", None)), out_specs=row_spec, check_vma=False)
```
